128 devices in a mesh: row: 8 (over z, core), col: 16 (over x, y).
Axes of the slice: x: 4, y: 4, z: 4, core: 2. Of those that a mesh axis runs over, the one named last changes fastest.
Arguments:
- right_side: float32 [16, 2048, 6144], P(None, 'row', 'col'), may hold values from -100 to 100
- cond_x: float32 [2048, 6144], P('row', 'col'), may hold values from 0.25 to 4
- cond_y: float32 [2048, 6144], P('row', 'col'), may hold values from 0.25 to 4
- pad_mask: int32 [2048, 6144], P('row', 'col'), may hold values 0 or 1
Outputs:
- solution: float32 [16, 2048, 6144], P(None, 'row', 'col')
- residual: float32 [16, 2048, 6144], P(None, 'row', 'col')
The draws below stay inside these ranges and needn't reach their ends.
All inputs are finite; a program needn't handle non-finite values. No bound on the sum of `pad_mask` on one device may be relied on, other than what follows from the above.
Results may differ from the reference program's by a relative error of at most 0.0003.
Values sent between devices are 32-bit elements; how exact they have to be, the bound alone decides.
A program may use at most 128 MiB of HBM per device.

```python
import math
import jax
import jax.numpy as jnp
from jax import lax

RHS = 16
ITERS = 3
NX = 2048
NY = 6144


def draw_right_side(key, part):
    key_rough = jax.random.fold_in(key, 11)
    key_scale = jax.random.fold_in(key, 12)
    row_pos = jnp.arange(NX, dtype=jnp.float32) / NX - 0.5
    col_pos = jnp.arange(NY, dtype=jnp.float32) / NY - 0.5
    pattern = jnp.exp(jax.random.uniform(key_scale, (RHS, 1, 1), jnp.float32, math.log(0.3), math.log(3.0)))
    roughness = jnp.clip(jax.random.normal(key_rough, (RHS, NX, NY), jnp.float32), -6.0, 6.0)
    growth = jnp.power(3.0, row_pos)[:, None] * jnp.power(3.0, col_pos)[None, :]
    return (pattern * growth[None] * roughness).astype(jnp.float32)


def place_ends(result, stream_key, low, high):
    longest = result.shape.index(max(result.shape))
    spots = []
    for shift in (0, 1):
        where = [jax.random.randint(jax.random.fold_in(stream_key, axis), (), 0, length) for axis, length in enumerate(result.shape)]
        where[longest] = (where[longest] + shift) % result.shape[longest]
        spots.append(tuple(where))
    return result.at[spots[0]].set(low).at[spots[1]].set(high)


def level_of(rng, extent, split, least, high):
    def one(dim, parts):
        steps = jax.random.uniform(jax.random.fold_in(jax.random.fold_in(rng, 6), dim), (parts,), jnp.float32, least / len(split), high / len(split))
        return jnp.repeat(jnp.exp(steps), extent[dim] // parts).reshape((-1,) + (1,) * (len(extent) - dim - 1))

    loudness = one(*split[0])
    for cut in split[1:]:
        loudness = loudness * one(*cut)
    return loudness


def setup_inputs(seed: int = 0) -> dict:
    key_of = jax.random.split(jax.random.key(seed), 5)
    right_side = draw_right_side(jax.random.fold_in(key_of[4], 71), 0)
    cond_x = jnp.clip(jnp.exp(math.log(4.0) - 2.7725887 * jax.random.uniform(key_of[1], (NX, NY), jnp.float32) ** level_of(key_of[1], (NX, NY), ((0, 8), (1, 16)), -0.2, 0.2)), 0.25, 4.0)
    cond_y = jnp.clip(jnp.exp(math.log(4.0) - 2.7725887 * jax.random.uniform(key_of[2], (NX, NY), jnp.float32) ** level_of(key_of[2], (NX, NY), ((0, 8), (1, 16)), -0.2, 0.2)), 0.25, 4.0)
    pad_mask = place_ends((jax.random.randint(key_of[3], (NX, NY), 0, 16) < 1).astype(jnp.int32), jax.random.fold_in(key_of[3], 1), 0, 1)
    return {"right_side": right_side, "cond_x": cond_x, "cond_y": cond_y, "pad_mask": pad_mask}


exact_precision = lax.Precision.HIGHEST

def neighbour_sum(padded, cond_x, cond_above, cond_y, cond_left):
    total = cond_x * padded[:, 2:, 1:-1] + cond_above * padded[:, :-2, 1:-1]
    return total + cond_y * padded[:, 1:-1, 2:] + cond_left * padded[:, 1:-1, :-2]

def gram(left, right):
    return jnp.einsum('kab,lab->kl', left, right, precision=exact_precision)

def combine(field, matrix):
    return jnp.einsum('kab,kl->lab', field, matrix, precision=exact_precision)

def small_solve(matrix, right):
    factor = jnp.linalg.cholesky(matrix)
    return jax.scipy.linalg.cho_solve((factor, True), right)

def reference(right_side, cond_x, cond_y, pad_mask):
    pad_nodes = pad_mask.astype(jnp.float32)
    free_nodes = 1.0 - pad_nodes
    cond_above = jnp.pad(cond_x, ((1, 0), (0, 0)))[:-1]
    cond_left = jnp.pad(cond_y, ((0, 0), (1, 0)))[:, :-1]
    diagonal = free_nodes * (cond_x + cond_above + cond_y + cond_left) + pad_nodes
    inverse = 1.0 / diagonal

    def operate(field):
        padded = jnp.pad(free_nodes * field, ((0, 0), (1, 1), (1, 1)))
        return pad_nodes * field + free_nodes * (diagonal * field - neighbour_sum(padded, cond_x, cond_above, cond_y, cond_left))
    solution = jnp.zeros_like(right_side)
    residual = right_side
    precond = residual * inverse
    direction = precond
    gram_now = gram(residual, precond)
    for iteration in range(ITERS):
        image = operate(direction)
        alpha_block = small_solve(gram(direction, image), gram_now)
        solution = solution + combine(direction, alpha_block)
        residual = residual - combine(image, alpha_block)
        precond = residual * inverse
        gram_next = gram(residual, precond)
        beta_block = small_solve(gram_now, gram_next)
        direction = precond + combine(direction, beta_block)
        gram_now = gram_next
    return (solution, residual)
```

```python
import functools

import jax
import jax.numpy as jnp
from jax import lax
from jax.experimental import pallas as pl
from jax.experimental.pallas import tpu as pltpu
from jax.sharding import PartitionSpec as P

RHS = 16
STEPS = 3
LANES = 128
MESH = pl.DeviceIdType.MESH
F32 = jnp.float32
BF16 = jnp.bfloat16
UNROLL = 8
GROUP = 64
ROWS = 32


def split(value):
    high = value.astype(BF16)
    return high, (value - high.astype(F32)).astype(BF16)


def lane_of(shape):
    return lax.broadcasted_iota(jnp.int32, shape, len(shape) - 1)


def tiles_of(value):
    return [value[:, c : c + LANES] for c in range(0, value.shape[1], LANES)]


def stay_scalar(flag):
    return jnp.where(flag, 1.0, 0.0).astype(F32)


def gram_dot(left, right):
    return lax.dot_general(left, right, (((1,), (1,)), ((), ())), preferred_element_type=F32)


def eliminate(stack, order):
    rows = stack.shape[0]
    lane = lane_of((1, LANES))
    start = 0
    for p in range(order):
        keep = p // 8 * 8
        if keep > start:
            stack = stack[keep - start :]
            start = keep
        row = stack[p - start : p - start + 1, :]
        pivot = row[:, p : p + 1]
        col = stack[:, p : p + 1] / pivot
        stack = jnp.where(lane == p, col, stack - col * row)
    return stack[order - start :]


def main_kernel(grid, rhs, cx_in, cy_in, pad_in, ub0, ub1, ub2, ub3, lhs, dm, dp,
                cx, cy, pad, s, u0, u1, u2, bx, by, natural, byl, pk, cyh, sh, upk, uh, gsend, ga, gb,
                in_sem, bar_send, bar_recv):
    nrow, ncol = grid
    rb, cb = dm.shape
    nb = rb // LANES
    row, col = lax.axis_index("row"), lax.axis_index("col")
    down, above = lax.rem(row + 1, nrow), lax.rem(row + nrow - 1, nrow)
    right, left = lax.rem(col + 1, ncol), lax.rem(col + ncol - 1, ncol)
    fields = [u0, u1, u2]
    basis = [ub0, ub1, ub2, ub3]
    used = [0]
    sent = []

    def send(src, dst, row_to, col_to):
        slot = used[0]
        used[0] += 1
        copy = pltpu.make_async_remote_copy(
            src_ref=src, dst_ref=dst, send_sem=bar_send.at[slot], recv_sem=bar_recv.at[slot],
            device_id=(row_to, col_to), device_id_type=MESH)
        copy.start()
        sent.append(copy)
        return copy

    local = []
    for n, (src, dst) in enumerate(((cy_in, cy), (cx_in, cx.at[pl.ds(8, rb)]), (pad_in, pad))):
        copy = pltpu.make_async_copy(src, dst, in_sem.at[n])
        copy.start()
        local.append(copy)
    fill = []
    for k in range(RHS):
        copy = pltpu.make_async_copy(rhs.at[k], u0.at[pl.ds(1, rb), k, :], in_sem.at[3 + k])
        copy.start()
        fill.append(copy)

    barrier = pltpu.get_barrier_semaphore()
    for d in range(1, nrow):
        pl.semaphore_signal(barrier, inc=1, device_id=(lax.rem(row + d, nrow), col), device_id_type=MESH)
    for d in range(1, ncol):
        pl.semaphore_signal(barrier, inc=1, device_id=(row, lax.rem(col + d, ncol)), device_id_type=MESH)

    local[0].wait()
    pk[0] = jnp.transpose(cy[:, cb - LANES :])[LANES - 8 :]
    local[1].wait()
    pl.semaphore_wait(barrier, nrow + ncol - 2)
    got_cx = send(cx.at[pl.ds(rb, 8)], cx.at[pl.ds(0, 8)], down, col)
    got_cy = send(pk.at[0], cyh, row, right)
    local[2].wait()
    got_cx.wait_recv()
    got_cy.wait_recv()
    cx[0:8] = cx[0:8] * stay_scalar(row > 0)
    cyh[...] = cyh[...] * stay_scalar(col > 0)
    natural[...] = jnp.transpose(jnp.broadcast_to(cyh[7:8, :], (LANES, rb)))
    chunk = 32
    for r in range(0, rb, chunk):
        here = pl.ds(r, chunk)
        cond_y = cy[here]
        rolled = pltpu.roll(cond_y, 1, axis=1)
        first = jnp.where(lane_of((chunk, LANES)) == 0, natural[here], rolled[:, :LANES])
        cond_left = jnp.concatenate([first, rolled[:, LANES:]], axis=1)
        pads = pad[here].astype(F32)
        free = 1.0 - pads
        diagonal = free * (cx[pl.ds(r + 8, chunk)] + cx[pl.ds(r + 7, chunk)] + cond_y + cond_left) + pads
        root = lax.rsqrt(diagonal)
        dm[here] = root
        dp[here] = diagonal * root
        s[pl.ds(r + 8, chunk)] = free * root
    pk[1] = jnp.transpose(s[pl.ds(8, rb), 0:LANES])[:8]
    pk[2] = jnp.transpose(s[pl.ds(8, rb), cb - LANES : cb])[LANES - 8 :]
    got_s = [
        send(s.at[pl.ds(rb, 8)], s.at[pl.ds(0, 8)], down, col),
        send(s.at[pl.ds(8, 8)], s.at[pl.ds(rb + 8, 8)], above, col),
        send(pk.at[1], sh.at[1], row, left),
        send(pk.at[2], sh.at[0], row, right),
    ]

    def send_edges(j):
        field = fields[j]
        return [
            send(field.at[rb], field.at[0], down, col),
            send(field.at[1], field.at[rb + 1], above, col),
            send(upk.at[j, 0], uh.at[j, 1], row, left),
            send(upk.at[j, 1], uh.at[j, 0], row, right),
        ]

    lane = lane_of((RHS, LANES))

    def store_split(j, r, value):
        high, low = split(value)
        basis[j][r, :RHS, :] = high
        basis[j][r, RHS:, :] = low

    def pack_edges(value, r, held):
        low, high = held
        low = jnp.where(lane == r, pltpu.roll(value[:, :LANES], r, axis=1), low)
        high = jnp.where(lane == r, pltpu.roll(value[:, cb - LANES :], lax.rem(r + 1, LANES), axis=1), high)
        return low, high

    empty = (jnp.zeros((RHS, LANES), F32), jnp.zeros((RHS, LANES), F32))

    for copy in fill:
        copy.wait()
    for b in range(nb):
        def begin(i, held, b=b):
            for t in range(UNROLL):
                r = i * UNROLL + t
                at = b * LANES + r
                value = u0[at + 1] * dm[pl.ds(at, 1), :]
                u0[at + 1] = value
                store_split(0, at, value)
                held = pack_edges(value, r, held)
            return held

        low, high = lax.fori_loop(0, LANES // UNROLL, begin, empty)
        upk[0, 0, b] = low
        upk[0, 1, b] = high
    got_u = send_edges(0)

    lows = STEPS + 1

    def gram_loop(left_blocks, right_blocks):
        height = len(left_blocks) * RHS
        width = len(right_blocks) * RHS

        def body(i, total):
            rows = [i * GROUP + t for t in range(GROUP)]

            def operand(blocks):
                parts = [
                    jnp.concatenate(
                        [basis[n % lows][r, n // lows * RHS : (n // lows + 1) * RHS, :] for n in blocks], axis=0)
                    for r in rows
                ]
                return jnp.concatenate(parts, axis=1)

            return total + gram_dot(operand(left_blocks), operand(right_blocks))

        return lax.fori_loop(0, rb // GROUP, body, jnp.zeros((height, width), F32))

    def keep_moment(k, value):
        gsend[0, :, k * RHS : (k + 1) * RHS] = value

    gsend[...] = jnp.zeros_like(gsend)
    total = gram_loop([0], [0, lows])
    keep_moment(0, total[:, :RHS] + 2.0 * total[:, RHS:])

    for copy in got_s:
        copy.wait_recv()
    s[pl.ds(rb + 8, 8)] = s[pl.ds(rb + 8, 8)] * stay_scalar(row < nrow - 1)
    sh[1] = sh[1] * stay_scalar(col < ncol - 1)
    byl[...] = jnp.broadcast_to(cyh[7:8, :] * sh[0, 7:8, :] * pk[1, 0:1, :], (8, rb))
    natural[...] = jnp.transpose(jnp.broadcast_to(sh[1, 0:1, :], (LANES, rb)))
    for r in range(0, rb, chunk):
        here = pl.ds(r, chunk)
        mine = s[pl.ds(r + 8, chunk)]
        rolled = pltpu.roll(mine, cb - 1, axis=1)
        last = jnp.where(lane_of((chunk, LANES)) == LANES - 1, natural[here], rolled[:, cb - LANES :])
        following = jnp.concatenate([rolled[:, : cb - LANES], last], axis=1)
        by[here] = cy[here] * mine * following
        bx[here] = cx[pl.ds(r + 7, chunk)] * s[pl.ds(r + 7, chunk)] * mine
    bx[rb : rb + 1] = cx[rb + 7 : rb + 8] * s[rb + 7 : rb + 8] * s[rb + 8 : rb + 9]

    for j in range(STEPS):
        for copy in got_u:
            copy.wait_recv()
        source = fields[j]
        final = j == STEPS - 1
        for b in range(nb):
            from_left = uh[j, 0, b] * byl[0:1, b * LANES : (b + 1) * LANES]
            from_right = uh[j, 1, b]

            def apply(i, held, b=b, from_left=from_left, from_right=from_right, source=source, j=j, final=final):
                for t in range(UNROLL):
                    r = i * UNROLL + t
                    at = b * LANES + r
                    here = source[at + 1]
                    side = by[pl.ds(at, 1), :]
                    total = bx[pl.ds(at, 1), :] * source[at] + bx[pl.ds(at + 1, 1), :] * source[at + 2]
                    ahead = [pltpu.roll(v, LANES - 1, axis=1) for v in tiles_of(here)]
                    ahead.append(pltpu.roll(from_right, LANES - 1 - r, axis=1))
                    ahead = [jnp.where(lane == LANES - 1, ahead[c + 1], ahead[c]) for c in range(len(ahead) - 1)]
                    behind = [pltpu.roll(v, 1, axis=1) for v in tiles_of(side * here)]
                    behind.insert(0, pltpu.roll(from_left, lax.rem(LANES - r, LANES), axis=1))
                    behind = [jnp.where(lane == 0, behind[c], behind[c + 1]) for c in range(len(behind) - 1)]
                    value = total + side * jnp.concatenate(ahead, axis=1) + jnp.concatenate(behind, axis=1)
                    store_split(j + 1, at, value)
                    if not final:
                        fields[j + 1][at + 1] = value
                        held = pack_edges(value, r, held)
                return held

            low, high = lax.fori_loop(0, LANES // UNROLL, apply, empty)
            if not final:
                upk[j + 1, 0, b] = low
                upk[j + 1, 1, b] = high
        if not final:
            got_u = send_edges(j + 1)
            total = gram_loop([j, lows + j, j + 1], [j + 1, lows + j + 1])
            even = total[2 * RHS :]
            keep_moment(2 * j + 2, even[:, :RHS] + 2.0 * even[:, RHS:])
        else:
            total = gram_loop([j, lows + j], [j + 1, lows + j + 1])
        keep_moment(2 * j + 1, total[:RHS, :RHS] + total[:RHS, RHS:] + total[RHS : 2 * RHS, :RHS])

    def reduce_over(size, me, slots, n, place):
        got = []
        for d in range(1, size):
            to = lax.rem(me + d, size)
            got.append(send(gsend.at[n], slots.at[me], *place(to)))
        slots[me] = gsend[n]
        for copy in got:
            copy.wait_recv()
        total = slots[0]
        for n in range(1, size):
            total = total + slots[n]
        return total

    gsend[1] = reduce_over(nrow, row, ga, 0, lambda to: (to, col))
    total = reduce_over(ncol, col, gb, 1, lambda to: (row, to))

    wide = lane_of((RHS, LANES))
    turned = jnp.transpose(total)
    turned = jnp.concatenate([turned[k * RHS : (k + 1) * RHS] for k in range(LANES // RHS)], axis=1)
    moments = 0.5 * (total + turned)
    stiff = moments - pltpu.roll(moments, LANES - RHS, axis=1)
    order = STEPS * RHS
    blocks = [stiff] + [pltpu.roll(stiff, LANES - RHS * n, axis=1) for n in range(1, STEPS)] + [moments]
    stack = jnp.concatenate([jnp.where(wide < order, v, 0.0) for v in blocks], axis=0)
    solved = eliminate(stack, order)
    unit = jnp.where(wide == lax.broadcasted_iota(jnp.int32, (RHS, LANES), 0), 1.0, 0.0)
    remain = unit - solved + pltpu.roll(solved, RHS, axis=1)
    coef = jnp.concatenate([solved, remain], axis=0)
    high = coef.astype(BF16).astype(F32)
    low = coef - high
    lhs[...] = jnp.concatenate([high + pltpu.roll(high, LANES // 2, axis=1), low], axis=0).astype(BF16)

    for copy in sent:
        copy.wait_send()


def combine_kernel(ub0, ub1, ub2, ub3, lhs, dm, dp, x_out, r_out, x_buf, r_buf, sem):
    rb, cb = dm.shape
    block = 64
    coef = lhs[...]
    started = []
    for n in range(rb // block):
        def body(i, carry, n=n):
            rows = [n * block + i * ROWS + t for t in range(ROWS)]
            out = jnp.dot(coef, jnp.concatenate(
                [
                    jnp.concatenate([v[r, m : m + RHS, :] for m in (0, RHS) for v in (ub0, ub1, ub2, ub3)], axis=0)
                    for r in rows
                ], axis=1), preferred_element_type=F32)
            for t, r in enumerate(rows):
                part = out[:, t * cb : (t + 1) * cb]
                x_buf[r] = (part[:RHS] + part[2 * RHS : 3 * RHS]) * dm[pl.ds(r, 1), :]
                r_buf[r] = (part[RHS : 2 * RHS] + part[3 * RHS :]) * dp[pl.ds(r, 1), :]
            return carry

        lax.fori_loop(0, block // ROWS, body, 0)
        here = pl.ds(n * block, block)
        for k in range(RHS):
            for m, (buf, out) in enumerate(((x_buf, x_out), (r_buf, r_out))):
                copy = pltpu.make_async_copy(buf.at[here, k, :], out.at[k, here, :], sem.at[n, m, k])
                copy.start()
                started.append(copy)
    for copy in started:
        copy.wait()


def shards(nrow, ncol, right_side, cond_x, cond_y, pad_mask):
    rb, cb = cond_x.shape
    nb = rb // LANES
    sends = 2 + 4 + 4 * STEPS + (nrow - 1) + (ncol - 1)
    hbm = pl.BlockSpec(memory_space=pltpu.HBM)
    vmem = pl.BlockSpec(memory_space=pltpu.VMEM)
    field = pltpu.VMEM((rb + 2, RHS, cb), F32)
    *kept, = pl.pallas_call(
        functools.partial(main_kernel, (nrow, ncol)),
        out_shape=(
            *[pltpu.VMEM((rb, 2 * RHS, cb), BF16)] * (STEPS + 1), pltpu.VMEM((4 * RHS, LANES), BF16),
            pltpu.VMEM((rb, cb), F32), pltpu.VMEM((rb, cb), F32),
        ),
        in_specs=[hbm] * 4,
        out_specs=(vmem,) * (STEPS + 4),
        scratch_shapes=[
            pltpu.VMEM((rb + 8, cb), F32), pltpu.VMEM((rb, cb), F32), pltpu.VMEM((rb, cb), jnp.int32),
            pltpu.VMEM((rb + 16, cb), F32), field, field, field,
            pltpu.VMEM((rb + 8, cb), F32), pltpu.VMEM((rb, cb), F32),
            pltpu.VMEM((rb, LANES), F32), pltpu.VMEM((8, rb), F32), pltpu.VMEM((3, 8, rb), F32),
            pltpu.VMEM((8, rb), F32), pltpu.VMEM((2, 8, rb), F32),
            pltpu.VMEM((STEPS, 2, nb, RHS, LANES), F32), pltpu.VMEM((STEPS, 2, nb, RHS, LANES), F32),
            pltpu.VMEM((2, RHS, LANES), F32), pltpu.VMEM((nrow, RHS, LANES), F32), pltpu.VMEM((ncol, RHS, LANES), F32),
            pltpu.SemaphoreType.DMA((3 + RHS,)), pltpu.SemaphoreType.DMA((sends,)), pltpu.SemaphoreType.DMA((sends,)),
        ],
        compiler_params=pltpu.CompilerParams(
            collective_id=0, has_side_effects=True, vmem_limit_bytes=24 * 2**20),
    )(*(pltpu.with_memory_space_constraint(v, pltpu.HBM) for v in (right_side, cond_x, cond_y, pad_mask)))
    out = jax.ShapeDtypeStruct((RHS, rb, cb), F32)
    return pl.pallas_call(
        combine_kernel,
        out_shape=(out, out),
        in_specs=[vmem] * (STEPS + 4),
        out_specs=(hbm, hbm),
        scratch_shapes=[
            pltpu.VMEM((rb, RHS, cb), F32), pltpu.VMEM((rb, RHS, cb), F32),
            pltpu.SemaphoreType.DMA((rb // 64, 2, RHS)),
        ],
        compiler_params=pltpu.CompilerParams(vmem_limit_bytes=14 * 2**20),
    )(*kept)


def solution(mesh):
    nrow, ncol = mesh.shape["row"], mesh.shape["col"]
    field, plane = P(None, "row", "col"), P("row", "col")
    return jax.shard_map(
        functools.partial(shards, nrow, ncol), mesh=mesh,
        in_specs=(field, plane, plane, plane), out_specs=(field, field), check_vma=False,
    )
```

```python
import functools

import jax
import jax.numpy as jnp
from jax import lax
from jax.experimental import pallas as pl
from jax.experimental.pallas import tpu as pltpu
from jax.sharding import PartitionSpec as P

RHS = 16
STEPS = 3
LANES = 128
MESH = pl.DeviceIdType.MESH
F32 = jnp.float32
BF16 = jnp.bfloat16
UNROLL = 16
BEGIN = 16
SHIFT = 64
GROUP = 64
ROWS = 64


def split(value):
    high = value.astype(BF16)
    return high, (value - high.astype(F32)).astype(BF16)


def lane_of(shape):
    return lax.broadcasted_iota(jnp.int32, shape, len(shape) - 1)


def tiles_of(value):
    return [value[:, c : c + LANES] for c in range(0, value.shape[1], LANES)]


def stay_scalar(flag):
    return jnp.where(flag, 1.0, 0.0).astype(F32)


def gram_dot(left, right):
    return lax.dot_general(left, right, (((1,), (1,)), ((), ())), preferred_element_type=F32)


def eliminate(stack, order, first):
    rows = stack.shape[0]
    lane = lane_of((1, LANES))
    start = 0
    for p in range(order):
        keep = p // 8 * 8
        if keep > start:
            stack = stack[keep - start :]
            start = keep
        row = stack[p - start : p - start + 1, :]
        at = first + p
        col = stack[:, at : at + 1] / row[:, at : at + 1]
        stack = jnp.where(lane == at, col, stack - col * row)
    return stack[order - start :]


def main_kernel(grid, rhs, cx_in, cy_in, pad_in, ub0, ub1, ub2, ub3, lhs, dm, dp, cxh,
                cx, cy, pad, s, u0, u1, bx, by, bys, natural, pk, cyh, sh, upk, uh, edge, rolled, turn, gsend, ga, gb,
                in_sem, bar_send, bar_recv):
    nrow, ncol = grid
    rb, cb = dm.shape
    nb = rb // LANES
    row, col = lax.axis_index("row"), lax.axis_index("col")
    down, above = lax.rem(row + 1, nrow), lax.rem(row + nrow - 1, nrow)
    right, left = lax.rem(col + 1, ncol), lax.rem(col + ncol - 1, ncol)
    fields = [u0, u1, u0]
    basis = [ub0, ub1, ub2, ub3]
    used = [0]
    sent = []

    def send(src, dst, row_to, col_to):
        slot = used[0]
        used[0] += 1
        copy = pltpu.make_async_remote_copy(
            src_ref=src, dst_ref=dst, send_sem=bar_send.at[slot], recv_sem=bar_recv.at[slot],
            device_id=(row_to, col_to), device_id_type=MESH)
        copy.start()
        sent.append(copy)
        return copy

    def done(copy):
        copy.wait_send()
        sent[:] = [c for c in sent if c is not copy]

    barrier = pltpu.get_barrier_semaphore()
    for d in range(1, nrow):
        pl.semaphore_signal(barrier, inc=1, device_id=(lax.rem(row + d, nrow), col), device_id_type=MESH)
    for d in range(1, ncol):
        pl.semaphore_signal(barrier, inc=1, device_id=(row, lax.rem(col + d, ncol)), device_id_type=MESH)

    local = []
    for n, (src, dst) in enumerate(((cy_in, cy), (cx_in, cx.at[pl.ds(8, rb)]), (pad_in, pad))):
        copy = pltpu.make_async_copy(src, dst, in_sem.at[n])
        copy.start()
        local.append(copy)
    fill = []
    for k in range(RHS):
        copy = pltpu.make_async_copy(rhs.at[k], u0.at[pl.ds(1, rb), k, :], in_sem.at[3 + k])
        copy.start()
        fill.append(copy)

    local[0].wait()
    pk[0] = jnp.transpose(cy[:, cb - LANES :])[LANES - 8 :]
    local[1].wait()
    pl.semaphore_wait(barrier, nrow + ncol - 2)
    got_cx = send(cx.at[pl.ds(rb, 8)], cxh, down, col)
    got_cy = send(pk.at[0], cyh, row, right)
    local[2].wait()
    cx[0:8] = jnp.zeros_like(cxh)
    chunk = 32

    def scale_nodes(r, height, width, left_known):
        here = pl.ds(r, height)
        cond_y = cy[here, :width]
        moved = pltpu.roll(cond_y, 1, axis=1)
        if left_known:
            first = jnp.where(lane_of((height, LANES)) == 0, natural[0, here], moved[:, :LANES])
            moved = jnp.concatenate([first, moved[:, LANES:]], axis=1) if width > LANES else first
        pads = pad[here, :width].astype(F32)
        free = 1.0 - pads
        diagonal = free * (cx[pl.ds(r + 8, height), :width] + cx[pl.ds(r + 7, height), :width] + cond_y + moved) + pads
        root = lax.rsqrt(diagonal)
        dm[here, :width] = root
        dp[here, :width] = diagonal * root
        s[pl.ds(r + 8, height), :width] = free * root

    for r in range(0, rb, chunk):
        scale_nodes(r, chunk, cb, False)

    lane = lane_of((RHS, LANES))

    def store_split(j, r, value, start=0):
        high, low = split(value)
        lanes = slice(start, start + value.shape[1])
        basis[j][r, :RHS, lanes] = high
        basis[j][r, RHS:, lanes] = low

    for copy in fill:
        copy.wait()
    rolled[0, 0] = u0[1]

    def inner(i, carry):
        for t in range(BEGIN):
            at = i * BEGIN + t
            value = u0[at + 1, :, LANES:] * dm[pl.ds(at, 1), :][:, LANES:]
            u0[at + 1, :, LANES:] = value
            store_split(0, at, value, LANES)
        return carry

    lax.fori_loop(0, rb // BEGIN, inner, 0)

    got_cx.wait_recv()
    got_cy.wait_recv()
    cx[0:8] = cxh[...] * stay_scalar(row > 0)
    cyh[...] = cyh[...] * stay_scalar(col > 0)
    natural[0] = jnp.transpose(jnp.broadcast_to(cyh[7:8, :], (LANES, rb)))
    scale_nodes(0, 8, cb, True)
    for r in range(0, rb, chunk):
        scale_nodes(r, chunk, LANES, True)
    pk[1] = jnp.transpose(s[pl.ds(8, rb), 0:LANES])[:8]
    pk[2] = jnp.transpose(s[pl.ds(8, rb), cb - LANES : cb])[LANES - 8 :]
    got_s = [
        send(s.at[pl.ds(rb, 8)], s.at[pl.ds(0, 8)], down, col),
        send(s.at[pl.ds(8, 8)], s.at[pl.ds(rb + 8, 8)], above, col),
        send(pk.at[1], sh.at[1], row, left),
        send(pk.at[2], sh.at[0], row, right),
    ]

    def send_edges(j):
        field = fields[j]
        return [
            send(field.at[rb], edge.at[j, 0], down, col),
            send(field.at[1], edge.at[j, 1], above, col),
            send(upk.at[j, 0], uh.at[j, 1], row, left),
            send(upk.at[j, 1], uh.at[j, 0], row, right),
        ]

    even_lane = (lane & 1) == 0

    def pack_edges(first, last, r, parity, held):
        ends = pltpu.roll(jnp.where(lane == LANES - 1, last, first), r, axis=1)
        here = (lane == r) | (lane == ((r - 1) & (LANES - 1)))
        return tuple(jnp.where(here, ends, held[n]) if n == parity else held[n] for n in range(2))

    def keep_edges(j, b, held):
        upk[j, 0, b] = jnp.where(even_lane, held[0], held[1])
        upk[j, 1, b] = jnp.where(even_lane, held[1], held[0])

    empty = (jnp.zeros((RHS, LANES), F32), jnp.zeros((RHS, LANES), F32))

    top = rolled[0, 0] * dm[0:1, :]
    u0[1, :, LANES:] = top[:, LANES:]
    store_split(0, 0, top[:, LANES:], LANES)
    for b in range(nb):
        def begin(i, held, b=b):
            for t in range(BEGIN):
                r = i * BEGIN + t
                at = b * LANES + r
                value = u0[at + 1, :, :LANES] * dm[pl.ds(at, 1), :][:, :LANES]
                u0[at + 1, :, :LANES] = value
                store_split(0, at, value)
                held = pack_edges(value, u0[at + 1, :, cb - LANES :], r, t % 2, held)
            return held

        keep_edges(0, b, lax.fori_loop(0, LANES // BEGIN, begin, empty))
    got_u = send_edges(0)

    lows = STEPS + 1

    def gram_loop(left_blocks, right_blocks):
        height = len(left_blocks) * RHS
        width = len(right_blocks) * RHS

        def body(i, total):
            rows = [i * GROUP + t for t in range(GROUP)]

            def operand(blocks):
                parts = [
                    jnp.concatenate(
                        [basis[n % lows][r, n // lows * RHS : (n // lows + 1) * RHS, :] for n in blocks], axis=0)
                    for r in rows
                ]
                return jnp.concatenate(parts, axis=1)

            return total + gram_dot(operand(left_blocks), operand(right_blocks))

        return lax.fori_loop(0, rb // GROUP, body, jnp.zeros((height, width), F32))

    def keep_moment(k, value):
        gsend[0 if k < 2 * STEPS - 1 else 2, :, k * RHS : (k + 1) * RHS] = value

    gsend[...] = jnp.zeros_like(gsend)
    place = lax.broadcasted_iota(jnp.int32, turn.shape, 0) & (LANES - 1)
    spot = lane_of(turn.shape)
    comes = jnp.where(spot < LANES, spot + 1, spot - 1) & (LANES - 1)
    turn[...] = jnp.where(place == comes, 1.0, 0.0).astype(BF16)
    total = gram_loop([0], [0, lows])
    keep_moment(0, total[:, :RHS] + 2.0 * total[:, RHS:])

    for copy in got_s:
        copy.wait_recv()
    s[pl.ds(rb + 8, 8)] = s[pl.ds(rb + 8, 8)] * stay_scalar(row < nrow - 1)
    sh[1] = sh[1] * stay_scalar(col < ncol - 1)
    natural[1] = jnp.transpose(jnp.broadcast_to(sh[0, 7:8, :], (LANES, rb)))
    natural[2] = jnp.transpose(jnp.broadcast_to(sh[1, 0:1, :], (LANES, rb)))
    for r in range(0, rb, chunk):
        here = pl.ds(r, chunk)
        mine = s[pl.ds(r + 8, chunk)]
        moved = pltpu.roll(mine, cb - 1, axis=1)
        last = jnp.where(lane_of((chunk, LANES)) == LANES - 1, natural[2, here], moved[:, cb - LANES :])
        side = cy[here] * mine * jnp.concatenate([moved[:, : cb - LANES], last], axis=1)
        by[here] = side
        moved = pltpu.roll(side, 1, axis=1)
        first = natural[0, here] * natural[1, here] * mine[:, :LANES]
        first = jnp.where(lane_of((chunk, LANES)) == 0, first, moved[:, :LANES])
        bys[here] = jnp.concatenate([first, moved[:, LANES:]], axis=1)
        bx[here] = cx[pl.ds(r + 7, chunk)] * s[pl.ds(r + 7, chunk)] * mine
    bx[rb : rb + 1] = cx[rb + 7 : rb + 8] * s[rb + 7 : rb + 8] * s[rb + 8 : rb + 9]

    def shift_loop(j, b):
        def body(i, carry):
            parts = []
            for t in range(SHIFT):
                at = b * LANES + i * SHIFT + t
                for c in range(0, cb, LANES):
                    parts.append(jnp.concatenate(
                        [basis[j][at, :RHS, c : c + LANES], basis[j][at, RHS:, c : c + LANES]], axis=1))
            out = jnp.dot(jnp.concatenate(parts, axis=0), turn[...], preferred_element_type=F32)
            n = 0
            for t in range(SHIFT):
                for c in range(0, cb, LANES):
                    for m in range(2):
                        rolled[i * SHIFT + t, m, :, c : c + LANES] = out[n : n + RHS, m * LANES : (m + 1) * LANES]
                    n += RHS
            return carry

        lax.fori_loop(0, LANES // SHIFT, body, 0)

    shift_loop(0, 0)
    def start_reduce(n, slots, turn_no, me, size, along_row):
        got = []
        for d in range(1, size):
            to = lax.rem(me + d, size)
            got.append(send(gsend.at[n], slots.at[turn_no, me], *((to, col) if along_row else (row, to))))
        slots[turn_no, me] = gsend[n]
        return got

    def finish_reduce(got, slots, turn_no, me, size):
        for copy in got:
            copy.wait_recv()
        total = slots[turn_no, 0]
        for n in range(1, size):
            total = total + slots[turn_no, n]
        return total

    for j in range(STEPS):
        if j == STEPS - 1:
            early = start_reduce(0, ga, 0, row, nrow, True)
        for copy in got_u:
            copy.wait_recv()
        for copy in got_u:
            done(copy)
        source = fields[j]
        source[0] = edge[j, 0]
        source[rb + 1] = edge[j, 1]
        final = j == STEPS - 1
        for b in range(nb):
            if b > 0:
                shift_loop(j, b)
                if final and b == 1:
                    gsend[1] = finish_reduce(early, ga, 0, row, nrow)
                    early = start_reduce(1, gb, 0, col, ncol, False)
            before = pltpu.roll(uh[j, 0, b], 1, axis=1)
            after = pltpu.roll(uh[j, 1, b], LANES - 1, axis=1)
            outside = (jnp.where(even_lane, before, after), jnp.where(even_lane, after, before))

            def apply(i, held, b=b, outside=outside, source=source, j=j, final=final):
                if not final:
                    for t in range(UNROLL):
                        r = (i - 1) * UNROLL + t
                        at = jnp.maximum(b * LANES + r, 0) + 1
                        first, last = fields[j + 1][at, :, :LANES], fields[j + 1][at, :, cb - LANES :]
                        held = pack_edges(first, last, r, t % 2, held)
                for t in range(UNROLL):
                    r = i * UNROLL + t
                    at = b * LANES + r
                    total = bx[pl.ds(at, 1), :] * source[at] + bx[pl.ds(at + 1, 1), :] * source[at + 2]
                    ends = pltpu.roll(outside[t % 2], (LANES - r) & (LANES - 1), axis=1)
                    ahead = tiles_of(rolled[r, 0]) + [ends]
                    ahead = [jnp.where(lane == LANES - 1, ahead[c + 1], ahead[c]) for c in range(len(ahead) - 1)]
                    behind = [ends] + tiles_of(rolled[r, 1])
                    behind = [jnp.where(lane == 0, behind[c], behind[c + 1]) for c in range(len(behind) - 1)]
                    total = total + by[pl.ds(at, 1), :] * jnp.concatenate(ahead, axis=1)
                    value = total + bys[pl.ds(at, 1), :] * jnp.concatenate(behind, axis=1)
                    store_split(j + 1, at, value)
                    if not final:
                        fields[j + 1][at + 1] = value
                return held

            held = lax.fori_loop(0, LANES // UNROLL, apply, empty)
            if not final:
                for t in range(UNROLL):
                    r = LANES - UNROLL + t
                    at = b * LANES + r + 1
                    first, last = fields[j + 1][at, :, :LANES], fields[j + 1][at, :, cb - LANES :]
                    held = pack_edges(first, last, r, t % 2, held)
                keep_edges(j + 1, b, held)
        if not final:
            got_u = send_edges(j + 1)
            total = gram_loop([j, lows + j, j + 1], [j + 1, lows + j + 1])
            shift_loop(j + 1, 0)
            even = total[2 * RHS :]
            keep_moment(2 * j + 2, even[:, :RHS] + 2.0 * even[:, RHS:])
        else:
            total = gram_loop([j, lows + j], [j + 1, lows + j + 1])
        keep_moment(2 * j + 1, total[:RHS, :RHS] + total[:RHS, RHS:] + total[RHS : 2 * RHS, :RHS])
    late = start_reduce(2, ga, 1, row, nrow, True)

    wide = lane_of((RHS, LANES))

    def turned(total):
        flip = jnp.transpose(total)
        flip = jnp.concatenate([flip[k * RHS : (k + 1) * RHS] for k in range(LANES // RHS)], axis=1)
        return 0.5 * (total + flip)

    moments = turned(finish_reduce(early, gb, 0, col, ncol))
    stiff = moments - pltpu.roll(moments, LANES - RHS, axis=1)
    order = STEPS * RHS
    blocks = [stiff] + [pltpu.roll(stiff, LANES - RHS * n, axis=1) for n in range(1, STEPS)] + [moments]
    stack = jnp.concatenate([jnp.where(wide < order, v, 0.0) for v in blocks], axis=0)
    stack = eliminate(stack, order - RHS, 0)
    gsend[3] = finish_reduce(late, ga, 1, row, nrow)
    late = start_reduce(3, gb, 1, col, ncol, False)
    last = turned(finish_reduce(late, gb, 1, col, ncol))
    last = jnp.where((wide >= order - RHS) & (wide < order), pltpu.roll(last, LANES - (STEPS * RHS), axis=1), 0.0)
    stack = jnp.concatenate([stack[:RHS] - last, stack[RHS:]], axis=0)
    solved = eliminate(stack, RHS, order - RHS)
    unit = jnp.where(wide == lax.broadcasted_iota(jnp.int32, (RHS, LANES), 0), 1.0, 0.0)
    remain = unit - solved + pltpu.roll(solved, RHS, axis=1)
    coef = jnp.concatenate([solved, remain], axis=0)
    high = coef.astype(BF16).astype(F32)
    low = coef - high
    lhs[...] = jnp.concatenate([high + pltpu.roll(high, LANES // 2, axis=1), low], axis=0).astype(BF16)

    for copy in sent:
        copy.wait_send()


def combine_kernel(ub0, ub1, ub2, ub3, lhs, dm, dp, x_out, r_out, x_buf, r_buf, sem):
    rb, cb = dm.shape
    block = 64
    coef = lhs[...]
    started = []
    for n in range(rb // block):
        def body(i, carry, n=n):
            rows = [n * block + i * ROWS + t for t in range(ROWS)]
            out = jnp.dot(coef, jnp.concatenate(
                [
                    jnp.concatenate([v[r, m : m + RHS, :] for m in (0, RHS) for v in (ub0, ub1, ub2, ub3)], axis=0)
                    for r in rows
                ], axis=1), preferred_element_type=F32)
            for t, r in enumerate(rows):
                part = out[:, t * cb : (t + 1) * cb]
                x_buf[r] = (part[:RHS] + part[2 * RHS : 3 * RHS]) * dm[pl.ds(r, 1), :]
                r_buf[r] = (part[RHS : 2 * RHS] + part[3 * RHS :]) * dp[pl.ds(r, 1), :]
            return carry

        lax.fori_loop(0, block // ROWS, body, 0)
        here = pl.ds(n * block, block)
        for k in range(RHS):
            for m, (buf, out) in enumerate(((x_buf, x_out), (r_buf, r_out))):
                copy = pltpu.make_async_copy(buf.at[here, k, :], out.at[k, here, :], sem.at[n, m, k])
                copy.start()
                started.append(copy)
    for copy in started:
        copy.wait()


def shards(nrow, ncol, right_side, cond_x, cond_y, pad_mask):
    rb, cb = cond_x.shape
    nb = rb // LANES
    sends = 2 + 4 + 4 * STEPS + 2 * (nrow - 1) + 2 * (ncol - 1)
    hbm = pl.BlockSpec(memory_space=pltpu.HBM)
    vmem = pl.BlockSpec(memory_space=pltpu.VMEM)
    field = pltpu.VMEM((rb + 2, RHS, cb), F32)
    *kept, = pl.pallas_call(
        functools.partial(main_kernel, (nrow, ncol)),
        out_shape=(
            *[pltpu.VMEM((rb, 2 * RHS, cb), BF16)] * (STEPS + 1), pltpu.VMEM((4 * RHS, LANES), BF16),
            pltpu.VMEM((rb, cb), F32), pltpu.VMEM((rb, cb), F32),
        ),
        in_specs=[hbm] * 4,
        out_specs=(vmem,) * (STEPS + 4),
        scratch_shapes=[
            pltpu.VMEM((8, cb), F32),
            pltpu.VMEM((rb + 8, cb), F32), pltpu.VMEM((rb, cb), F32), pltpu.VMEM((rb, cb), jnp.int32),
            pltpu.VMEM((rb + 16, cb), F32), field, field,
            pltpu.VMEM((rb + 8, cb), F32), pltpu.VMEM((rb, cb), F32), pltpu.VMEM((rb, cb), F32),
            pltpu.VMEM((3, rb, LANES), F32), pltpu.VMEM((3, 8, rb), F32),
            pltpu.VMEM((8, rb), F32), pltpu.VMEM((2, 8, rb), F32),
            pltpu.VMEM((STEPS, 2, nb, RHS, LANES), F32), pltpu.VMEM((STEPS, 2, nb, RHS, LANES), F32),
            pltpu.VMEM((STEPS, 2, RHS, cb), F32), pltpu.VMEM((LANES, 2, RHS, cb), F32), pltpu.VMEM((2 * LANES, 2 * LANES), BF16),
            pltpu.VMEM((4, RHS, LANES), F32), pltpu.VMEM((2, nrow, RHS, LANES), F32), pltpu.VMEM((2, ncol, RHS, LANES), F32),
            pltpu.SemaphoreType.DMA((3 + RHS,)), pltpu.SemaphoreType.DMA((sends,)), pltpu.SemaphoreType.DMA((sends,)),
        ],
        compiler_params=pltpu.CompilerParams(
            collective_id=0, has_side_effects=True, vmem_limit_bytes=24 * 2**20),
    )(*(pltpu.with_memory_space_constraint(v, pltpu.HBM) for v in (right_side, cond_x, cond_y, pad_mask)))
    out = jax.ShapeDtypeStruct((RHS, rb, cb), F32)
    return pl.pallas_call(
        combine_kernel,
        out_shape=(out, out),
        in_specs=[vmem] * (STEPS + 4),
        out_specs=(hbm, hbm),
        scratch_shapes=[
            pltpu.VMEM((rb, RHS, cb), F32), pltpu.VMEM((rb, RHS, cb), F32),
            pltpu.SemaphoreType.DMA((rb // 64, 2, RHS)),
        ],
        compiler_params=pltpu.CompilerParams(vmem_limit_bytes=14 * 2**20),
    )(*kept)


def solution(mesh):
    nrow, ncol = mesh.shape["row"], mesh.shape["col"]
    field, plane = P(None, "row", "col"), P("row", "col")
    return jax.shard_map(
        functools.partial(shards, nrow, ncol), mesh=mesh,
        in_specs=(field, plane, plane, plane), out_specs=(field, field), check_vma=False,
    )
```

```python
import functools

import jax
import jax.numpy as jnp
from jax import lax
from jax.experimental import pallas as pl
from jax.experimental.pallas import tpu as pltpu
from jax.sharding import PartitionSpec as P

RHS = 16
STEPS = 3
LANES = 128
MESH = pl.DeviceIdType.MESH
F32 = jnp.float32
BF16 = jnp.bfloat16
UNROLL = 16
BEGIN = 16
GROUP = 64
ROWS = 64


def split(value):
    high = value.astype(BF16)
    return high, (value - high.astype(F32)).astype(BF16)


def lane_of(shape):
    return lax.broadcasted_iota(jnp.int32, shape, len(shape) - 1)


def tiles_of(value):
    return [value[:, c : c + LANES] for c in range(0, value.shape[1], LANES)]


def stay_scalar(flag):
    return jnp.where(flag, 1.0, 0.0).astype(F32)


def gram_dot(left, right):
    return lax.dot_general(left, right, (((1,), (1,)), ((), ())), preferred_element_type=F32)


def eliminate(stack, order, first, panel=8):
    lane = lane_of((1, LANES))
    for start in range(0, order, panel):
        height = stack.shape[0]
        cols = [
            jnp.broadcast_to(stack[:, first + start + k : first + start + k + 1], (height, LANES)) for k in range(panel)
        ]
        for k in range(panel):
            scaled = cols[k] * (1.0 / cols[k][k : k + 1])
            stack = jnp.where(lane == first + start + k, scaled, stack - scaled * stack[k : k + 1])
            for m in range(k + 1, panel):
                cols[m] = cols[m] - scaled * cols[m][k : k + 1]
        stack = stack[panel:]
    return stack


def main_kernel(grid, rhs, cx_in, cy_in, pad_in, ub0, ub1, ub2, ub3, lhs, dm, dp, cxh,
                cx, cy, pad, s, u0, u1, bx, by, bys, natural, pk, cyh, sh, upk, uh, edge, rolled0, rolled1, turn, gsend, ga, gb, last_send, last_a, last_b,
                in_sem, bar_send, bar_recv):
    nrow, ncol = grid
    rb, cb = dm.shape
    nb = rb // LANES
    row, col = lax.axis_index("row"), lax.axis_index("col")
    down, above = lax.rem(row + 1, nrow), lax.rem(row + nrow - 1, nrow)
    right, left = lax.rem(col + 1, ncol), lax.rem(col + ncol - 1, ncol)
    fields = [u0, u1, u0]
    basis = [ub0, ub1, ub2, ub3]
    used = [0]
    sent = []

    def send(src, dst, row_to, col_to):
        slot = used[0]
        used[0] += 1
        copy = pltpu.make_async_remote_copy(
            src_ref=src, dst_ref=dst, send_sem=bar_send.at[slot], recv_sem=bar_recv.at[slot],
            device_id=(row_to, col_to), device_id_type=MESH)
        copy.start()
        sent.append(copy)
        return copy

    def done(copy):
        copy.wait_send()
        sent[:] = [c for c in sent if c is not copy]

    barrier = pltpu.get_barrier_semaphore()
    for d in range(1, nrow):
        pl.semaphore_signal(barrier, inc=1, device_id=(lax.rem(row + d, nrow), col), device_id_type=MESH)
    for d in range(1, ncol):
        pl.semaphore_signal(barrier, inc=1, device_id=(row, lax.rem(col + d, ncol)), device_id_type=MESH)

    local = []
    for n, (src, dst) in enumerate(((cy_in, cy), (cx_in, cx.at[pl.ds(8, rb)]), (pad_in, pad))):
        copy = pltpu.make_async_copy(src, dst, in_sem.at[n])
        copy.start()
        local.append(copy)
    fill = []
    for k in range(RHS):
        copy = pltpu.make_async_copy(rhs.at[k], u0.at[pl.ds(1, rb), k, :], in_sem.at[3 + k])
        copy.start()
        fill.append(copy)

    local[0].wait()
    pk[0] = jnp.transpose(cy[:, cb - LANES :])[LANES - 8 :]
    local[1].wait()
    pl.semaphore_wait(barrier, nrow + ncol - 2)
    got_cx = send(cx.at[pl.ds(rb, 8)], cxh, down, col)
    got_cy = send(pk.at[0], cyh, row, right)
    local[2].wait()
    cx[0:8] = jnp.zeros_like(cxh)
    chunk = 32

    def scale_nodes(r, height, width, left_known):
        here = pl.ds(r, height)
        cond_y = cy[here, :width]
        moved = pltpu.roll(cond_y, 1, axis=1)
        if left_known:
            first = jnp.where(lane_of((height, LANES)) == 0, natural[0, here], moved[:, :LANES])
            moved = jnp.concatenate([first, moved[:, LANES:]], axis=1) if width > LANES else first
        pads = pad[here, :width].astype(F32)
        free = 1.0 - pads
        diagonal = free * (cx[pl.ds(r + 8, height), :width] + cx[pl.ds(r + 7, height), :width] + cond_y + moved) + pads
        root = lax.rsqrt(diagonal)
        dm[here, :width] = root
        dp[here, :width] = diagonal * root
        s[pl.ds(r + 8, height), :width] = free * root

    for r in range(0, rb, chunk):
        scale_nodes(r, chunk, cb, False)

    lane = lane_of((RHS, LANES))

    def store_split(j, r, value, start=0):
        high, low = split(value)
        lanes = slice(start, start + value.shape[1])
        basis[j][r, :RHS, lanes] = high
        basis[j][r, RHS:, lanes] = low

    for copy in fill:
        copy.wait()
    rolled0[0, 0] = u0[1]

    def inner(i, carry):
        for t in range(BEGIN):
            at = i * BEGIN + t
            value = u0[at + 1, :, LANES:] * dm[pl.ds(at, 1), :][:, LANES:]
            u0[at + 1, :, LANES:] = value
            store_split(0, at, value, LANES)
        return carry

    lax.fori_loop(0, rb // BEGIN, inner, 0)

    got_cx.wait_recv()
    got_cy.wait_recv()
    cx[0:8] = cxh[...] * stay_scalar(row > 0)
    cyh[...] = cyh[...] * stay_scalar(col > 0)
    natural[0] = jnp.transpose(jnp.broadcast_to(cyh[7:8, :], (LANES, rb)))
    scale_nodes(0, 8, cb, True)
    for r in range(0, rb, chunk):
        scale_nodes(r, chunk, LANES, True)
    pk[1] = jnp.transpose(s[pl.ds(8, rb), 0:LANES])[:8]
    pk[2] = jnp.transpose(s[pl.ds(8, rb), cb - LANES : cb])[LANES - 8 :]
    got_s = [
        send(s.at[pl.ds(rb, 8)], s.at[pl.ds(0, 8)], down, col),
        send(s.at[pl.ds(8, 8)], s.at[pl.ds(rb + 8, 8)], above, col),
        send(pk.at[1], sh.at[1], row, left),
        send(pk.at[2], sh.at[0], row, right),
    ]

    def send_edges(j):
        field = fields[j]
        return [
            send(field.at[rb], edge.at[j, 0], down, col),
            send(field.at[1], edge.at[j, 1], above, col),
            send(upk.at[j, 0], uh.at[j, 1], row, left),
            send(upk.at[j, 1], uh.at[j, 0], row, right),
        ]

    even_lane = (lane & 1) == 0

    def pack_edges(first, last, r, parity, held):
        ends = pltpu.roll(jnp.where(lane == LANES - 1, last, first), r, axis=1)
        here = (lane == r) | (lane == ((r - 1) & (LANES - 1)))
        return tuple(jnp.where(here, ends, held[n]) if n == parity else held[n] for n in range(2))

    def keep_edges(j, b, held):
        upk[j, 0, b] = jnp.where(even_lane, held[0], held[1])
        upk[j, 1, b] = jnp.where(even_lane, held[1], held[0])

    empty = (jnp.zeros((RHS, LANES), F32), jnp.zeros((RHS, LANES), F32))

    top = rolled0[0, 0] * dm[0:1, :]
    u0[1, :, LANES:] = top[:, LANES:]
    store_split(0, 0, top[:, LANES:], LANES)
    for b in range(nb):
        def begin(i, held, b=b):
            for t in range(BEGIN):
                r = i * BEGIN + t
                at = b * LANES + r
                value = u0[at + 1, :, :LANES] * dm[pl.ds(at, 1), :][:, :LANES]
                u0[at + 1, :, :LANES] = value
                store_split(0, at, value)
                held = pack_edges(value, u0[at + 1, :, cb - LANES :], r, t % 2, held)
            return held

        keep_edges(0, b, lax.fori_loop(0, LANES // BEGIN, begin, empty))
    got_u = send_edges(0)

    lows = STEPS + 1

    def gram_rows(left_blocks, right_blocks, rows):
        def operand(blocks):
            parts = [
                jnp.concatenate(
                    [basis[n % lows][r, n // lows * RHS : (n // lows + 1) * RHS, :] for n in blocks], axis=0)
                for r in rows
            ]
            return jnp.concatenate(parts, axis=1)

        return gram_dot(operand(left_blocks), operand(right_blocks))

    def gram_loop(left_blocks, right_blocks):
        def body(i, total):
            return total + gram_rows(left_blocks, right_blocks, [i * GROUP + t for t in range(GROUP)])

        shape = (len(left_blocks) * RHS, len(right_blocks) * RHS)
        return lax.fori_loop(0, rb // GROUP, body, jnp.zeros(shape, F32))

    def keep_moment(k, value):
        if k < 2 * STEPS - 1:
            gsend[0, :, k * RHS : (k + 1) * RHS] = value
        else:
            gsend[2, :, :RHS] = value

    gsend[...] = jnp.zeros_like(gsend)
    place = lax.broadcasted_iota(jnp.int32, turn.shape, 0) & (LANES - 1)
    spot = lane_of(turn.shape)
    comes = jnp.where(spot < LANES, spot + 1, spot - 1) & (LANES - 1)
    turn[...] = jnp.where(place == comes, 1.0, 0.0).astype(BF16)
    total = gram_loop([0], [0, lows])
    keep_moment(0, total[:, :RHS] + 2.0 * total[:, RHS:])

    for copy in got_s:
        copy.wait_recv()
    s[pl.ds(rb + 8, 8)] = s[pl.ds(rb + 8, 8)] * stay_scalar(row < nrow - 1)
    sh[1] = sh[1] * stay_scalar(col < ncol - 1)
    natural[1] = jnp.transpose(jnp.broadcast_to(sh[0, 7:8, :], (LANES, rb)))
    natural[2] = jnp.transpose(jnp.broadcast_to(sh[1, 0:1, :], (LANES, rb)))
    for r in range(0, rb, chunk):
        here = pl.ds(r, chunk)
        mine = s[pl.ds(r + 8, chunk)]
        moved = pltpu.roll(mine, cb - 1, axis=1)
        last = jnp.where(lane_of((chunk, LANES)) == LANES - 1, natural[2, here], moved[:, cb - LANES :])
        side = cy[here] * mine * jnp.concatenate([moved[:, : cb - LANES], last], axis=1)
        by[here] = side
        moved = pltpu.roll(side, 1, axis=1)
        first = natural[0, here] * natural[1, here] * mine[:, :LANES]
        first = jnp.where(lane_of((chunk, LANES)) == 0, first, moved[:, :LANES])
        bys[here] = jnp.concatenate([first, moved[:, LANES:]], axis=1)
        bx[here] = cx[pl.ds(r + 7, chunk)] * s[pl.ds(r + 7, chunk)] * mine
    bx[rb : rb + 1] = cx[rb + 7 : rb + 8] * s[rb + 7 : rb + 8] * s[rb + 8 : rb + 9]

    def shift_rows(j, start, rolled):
        parts = []
        for t in range(UNROLL):
            for c in range(0, cb, LANES):
                parts.append(jnp.concatenate(
                    [basis[j][start + t, :RHS, c : c + LANES], basis[j][start + t, RHS:, c : c + LANES]], axis=1))
        out = jnp.dot(jnp.concatenate(parts, axis=0), turn[...], preferred_element_type=F32)
        n = 0
        for t in range(UNROLL):
            for c in range(0, cb, LANES):
                for m in range(2):
                    rolled[t, m, :, c : c + LANES] = out[n : n + RHS, m * LANES : (m + 1) * LANES]
                n += RHS

    shift_rows(0, 0, rolled0)

    def start_reduce(part, slots, me, size, along_row):
        got = []
        for d in range(1, size):
            to = lax.rem(me + d, size)
            got.append(send(part, slots.at[me], *((to, col) if along_row else (row, to))))
        slots[me] = part[...]
        return got

    def finish_reduce(got, slots, size):
        for copy in got:
            copy.wait_recv()
        parts = [slots[n] for n in range(size)]
        while len(parts) > 1:
            parts = [parts[n] + parts[n + 1] for n in range(0, len(parts), 2)]
        return parts[0]

    for j in range(STEPS):
        if j == STEPS - 1:
            early = start_reduce(gsend.at[0], ga, row, nrow, True)
        for copy in got_u:
            copy.wait_recv()
        for copy in got_u:
            done(copy)
        source = fields[j]
        source[0] = edge[j, 0]
        source[rb + 1] = edge[j, 1]
        final = j == STEPS - 1
        pair = jnp.zeros((2 * RHS, 2 * RHS), F32)
        for b in range(nb):
            if final and b == 1:
                gsend[1] = finish_reduce(early, ga, nrow)
                early = start_reduce(gsend.at[1], gb, col, ncol, False)
            before = pltpu.roll(uh[j, 0, b], 1, axis=1)
            after = pltpu.roll(uh[j, 1, b], LANES - 1, axis=1)
            outside = (jnp.where(even_lane, before, after), jnp.where(even_lane, after, before))

            def apply(i, held, b=b, outside=outside, source=source, j=j, final=final):
                held = list(held)
                base = b * LANES + i * 2 * UNROLL
                if final:
                    ready = jnp.maximum(base - 2 * UNROLL, 0)
                    fresh = gram_rows([j, lows + j], [j + 1, lows + j + 1], [ready + t for t in range(2 * UNROLL)])
                    held[0] = held[0] + jnp.where(base > 0, fresh, 0.0)
                else:
                    for t in range(2 * UNROLL):
                        r = (i - 1) * 2 * UNROLL + t
                        at = jnp.maximum(b * LANES + r, 0) + 1
                        first, last = fields[j + 1][at, :, :LANES], fields[j + 1][at, :, cb - LANES :]
                        held = pack_edges(first, last, r, t % 2, held)
                for half, (now, later) in enumerate(((rolled0, rolled1), (rolled1, rolled0))):
                    shift_rows(j, jnp.minimum(base + (half + 1) * UNROLL, rb - UNROLL), later)
                    for t in range(UNROLL):
                        r = (i * 2 + half) * UNROLL + t
                        at = b * LANES + r
                        total = bx[pl.ds(at, 1), :] * source[at] + bx[pl.ds(at + 1, 1), :] * source[at + 2]
                        ends = pltpu.roll(outside[t % 2], (LANES - r) & (LANES - 1), axis=1)
                        ahead = tiles_of(now[t, 0]) + [ends]
                        ahead = [jnp.where(lane == LANES - 1, ahead[c + 1], ahead[c]) for c in range(len(ahead) - 1)]
                        behind = [ends] + tiles_of(now[t, 1])
                        behind = [jnp.where(lane == 0, behind[c], behind[c + 1]) for c in range(len(behind) - 1)]
                        total = total + by[pl.ds(at, 1), :] * jnp.concatenate(ahead, axis=1)
                        value = total + bys[pl.ds(at, 1), :] * jnp.concatenate(behind, axis=1)
                        store_split(j + 1, at, value)
                        if not final:
                            fields[j + 1][at + 1] = value
                return tuple(held)

            trips = LANES // (2 * UNROLL)
            if final:
                pair, = lax.fori_loop(0, trips, apply, (pair,))
            else:
                held = lax.fori_loop(0, trips, apply, empty)
                for t in range(2 * UNROLL):
                    r = LANES - 2 * UNROLL + t
                    at = b * LANES + r + 1
                    first, last = fields[j + 1][at, :, :LANES], fields[j + 1][at, :, cb - LANES :]
                    held = pack_edges(first, last, r, t % 2, held)
                keep_edges(j + 1, b, held)
        if not final:
            got_u = send_edges(j + 1)
            total = gram_loop([j, lows + j, j + 1], [j + 1, lows + j + 1])
            shift_rows(j + 1, 0, rolled0)
            even = total[2 * RHS :]
            keep_moment(2 * j + 2, even[:, :RHS] + 2.0 * even[:, RHS:])
        else:
            rows = [rb - 2 * UNROLL + t for t in range(2 * UNROLL)]
            total = pair + gram_rows([j, lows + j], [j + 1, lows + j + 1], rows)
        keep_moment(2 * j + 1, total[:RHS, :RHS] + total[:RHS, RHS:] + total[RHS : 2 * RHS, :RHS])
    half = RHS // 2
    spread = pltpu.roll(gsend[2], 0, axis=1, stride=RHS, stride_axis=0)
    last_send[0] = jnp.concatenate(
        [jnp.sum(spread[n : n + half], axis=0, keepdims=True) for n in (0, half)], axis=0)
    late = start_reduce(last_send.at[0], last_a, row, nrow, True)

    wide = lane_of((RHS, LANES))

    def turned(total):
        flip = jnp.transpose(total)
        flip = jnp.concatenate([flip[k * RHS : (k + 1) * RHS] for k in range(LANES // RHS)], axis=1)
        return 0.5 * (total + flip)

    moments = turned(finish_reduce(early, gb, ncol))
    stiff = moments - pltpu.roll(moments, LANES - RHS, axis=1)
    order = STEPS * RHS
    blocks = [stiff] + [pltpu.roll(stiff, LANES - RHS * n, axis=1) for n in range(1, STEPS)] + [moments]
    stack = jnp.concatenate([jnp.where(wide < order, v, 0.0) for v in blocks], axis=0)
    stack = eliminate(stack, order - RHS, 0)
    last_send[1] = finish_reduce(late, last_a, nrow)
    late = start_reduce(last_send.at[1], last_b, col, ncol, False)
    last = finish_reduce(late, last_b, ncol)
    backward = [
        pltpu.roll(jnp.broadcast_to(last[n : n + 1], (half, LANES)), RHS, axis=1, stride=RHS, stride_axis=0)
        for n in range(2)
    ]
    last = jnp.concatenate([v[half - 1 - n : half - n] for v in backward for n in range(half)], axis=0)
    last = turned(last)
    inside = (wide >= order - RHS) & (wide < order)
    last = jnp.where(inside, pltpu.roll(last, order - RHS, axis=1), 0.0)
    stack = jnp.concatenate([stack[:RHS] - last, stack[RHS:]], axis=0)
    solved = eliminate(stack, RHS, order - RHS)
    unit = jnp.where(wide == lax.broadcasted_iota(jnp.int32, (RHS, LANES), 0), 1.0, 0.0)
    remain = unit - solved + pltpu.roll(solved, RHS, axis=1)
    coef = jnp.concatenate([solved, remain], axis=0)
    high = coef.astype(BF16).astype(F32)
    low = coef - high
    lhs[...] = jnp.concatenate([high + pltpu.roll(high, LANES // 2, axis=1), low], axis=0).astype(BF16)

    for copy in sent:
        copy.wait_send()


def combine_kernel(ub0, ub1, ub2, ub3, lhs, dm, dp, x_out, r_out, x_buf, r_buf, sem):
    rb, cb = dm.shape
    block = 64
    coef = lhs[...]
    started = []
    for n in range(rb // block):
        def body(i, carry, n=n):
            rows = [n * block + i * ROWS + t for t in range(ROWS)]
            out = jnp.dot(coef, jnp.concatenate(
                [
                    jnp.concatenate([v[r, m : m + RHS, :] for m in (0, RHS) for v in (ub0, ub1, ub2, ub3)], axis=0)
                    for r in rows
                ], axis=1), preferred_element_type=F32)
            for t, r in enumerate(rows):
                part = out[:, t * cb : (t + 1) * cb]
                x_buf[r] = (part[:RHS] + part[2 * RHS : 3 * RHS]) * dm[pl.ds(r, 1), :]
                r_buf[r] = (part[RHS : 2 * RHS] + part[3 * RHS :]) * dp[pl.ds(r, 1), :]
            return carry

        lax.fori_loop(0, block // ROWS, body, 0)
        here = pl.ds(n * block, block)
        for k in range(RHS):
            for m, (buf, out) in enumerate(((x_buf, x_out), (r_buf, r_out))):
                copy = pltpu.make_async_copy(buf.at[here, k, :], out.at[k, here, :], sem.at[n, m, k])
                copy.start()
                started.append(copy)
    for copy in started:
        copy.wait()


def shards(nrow, ncol, right_side, cond_x, cond_y, pad_mask):
    rb, cb = cond_x.shape
    nb = rb // LANES
    sends = 2 + 4 + 4 * STEPS + 2 * (nrow - 1) + 2 * (ncol - 1)
    hbm = pl.BlockSpec(memory_space=pltpu.HBM)
    vmem = pl.BlockSpec(memory_space=pltpu.VMEM)
    field = pltpu.VMEM((rb + 2, RHS, cb), F32)
    *kept, = pl.pallas_call(
        functools.partial(main_kernel, (nrow, ncol)),
        out_shape=(
            *[pltpu.VMEM((rb, 2 * RHS, cb), BF16)] * (STEPS + 1), pltpu.VMEM((4 * RHS, LANES), BF16),
            pltpu.VMEM((rb, cb), F32), pltpu.VMEM((rb, cb), F32),
        ),
        in_specs=[hbm] * 4,
        out_specs=(vmem,) * (STEPS + 4),
        scratch_shapes=[
            pltpu.VMEM((8, cb), F32),
            pltpu.VMEM((rb + 8, cb), F32), pltpu.VMEM((rb, cb), F32), pltpu.VMEM((rb, cb), jnp.int32),
            pltpu.VMEM((rb + 16, cb), F32), field, field,
            pltpu.VMEM((rb + 8, cb), F32), pltpu.VMEM((rb, cb), F32), pltpu.VMEM((rb, cb), F32),
            pltpu.VMEM((3, rb, LANES), F32), pltpu.VMEM((3, 8, rb), F32),
            pltpu.VMEM((8, rb), F32), pltpu.VMEM((2, 8, rb), F32),
            pltpu.VMEM((STEPS, 2, nb, RHS, LANES), F32), pltpu.VMEM((STEPS, 2, nb, RHS, LANES), F32),
            pltpu.VMEM((STEPS, 2, RHS, cb), F32), pltpu.VMEM((UNROLL, 2, RHS, cb), F32), pltpu.VMEM((UNROLL, 2, RHS, cb), F32),
            pltpu.VMEM((2 * LANES, 2 * LANES), BF16),
            pltpu.VMEM((3, RHS, LANES), F32), pltpu.VMEM((nrow, RHS, LANES), F32), pltpu.VMEM((ncol, RHS, LANES), F32),
            pltpu.VMEM((2, 2, LANES), F32), pltpu.VMEM((nrow, 2, LANES), F32), pltpu.VMEM((ncol, 2, LANES), F32),
            pltpu.SemaphoreType.DMA((3 + RHS,)), pltpu.SemaphoreType.DMA((sends,)), pltpu.SemaphoreType.DMA((sends,)),
        ],
        compiler_params=pltpu.CompilerParams(
            collective_id=0, has_side_effects=True, vmem_limit_bytes=24 * 2**20),
    )(*(pltpu.with_memory_space_constraint(v, pltpu.HBM) for v in (right_side, cond_x, cond_y, pad_mask)))
    out = jax.ShapeDtypeStruct((RHS, rb, cb), F32)
    return pl.pallas_call(
        combine_kernel,
        out_shape=(out, out),
        in_specs=[vmem] * (STEPS + 4),
        out_specs=(hbm, hbm),
        scratch_shapes=[
            pltpu.VMEM((rb, RHS, cb), F32), pltpu.VMEM((rb, RHS, cb), F32),
            pltpu.SemaphoreType.DMA((rb // 64, 2, RHS)),
        ],
        compiler_params=pltpu.CompilerParams(vmem_limit_bytes=14 * 2**20),
    )(*kept)


def solution(mesh):
    nrow, ncol = mesh.shape["row"], mesh.shape["col"]
    field, plane = P(None, "row", "col"), P("row", "col")
    return jax.shard_map(
        functools.partial(shards, nrow, ncol), mesh=mesh,
        in_specs=(field, plane, plane, plane), out_specs=(field, field), check_vma=False,
    )
```

```python
import functools

import jax
import jax.numpy as jnp
from jax import lax
from jax.experimental import pallas as pl
from jax.experimental.pallas import tpu as pltpu
from jax.sharding import PartitionSpec as P

RHS = 16
STEPS = 3
LANES = 128
MESH = pl.DeviceIdType.MESH
F32 = jnp.float32
BF16 = jnp.bfloat16
UNROLL = 16
BEGIN = 16
GROUP = 64
ROWS = 64


def split(value):
    high = value.astype(BF16)
    return high, (value - high.astype(F32)).astype(BF16)


def lane_of(shape):
    return lax.broadcasted_iota(jnp.int32, shape, len(shape) - 1)


def tiles_of(value):
    return [value[:, c : c + LANES] for c in range(0, value.shape[1], LANES)]


def stay_scalar(flag):
    return jnp.where(flag, 1.0, 0.0).astype(F32)


def gram_dot(left, right):
    return lax.dot_general(left, right, (((1,), (1,)), ((), ())), preferred_element_type=F32)


def eliminate(stack, order, first, panel=8):
    lane = lane_of((1, LANES))
    for start in range(0, order, panel):
        height = stack.shape[0]
        cols = [
            jnp.broadcast_to(stack[:, first + start + k : first + start + k + 1], (height, LANES)) for k in range(panel)
        ]
        for k in range(panel):
            scaled = cols[k] * (1.0 / cols[k][k : k + 1])
            stack = jnp.where(lane == first + start + k, scaled, stack - scaled * stack[k : k + 1])
            for m in range(k + 1, panel):
                cols[m] = cols[m] - scaled * cols[m][k : k + 1]
        stack = stack[panel:]
    return stack


def main_kernel(grid, rhs, cx_in, cy_in, pad_in, ub0, ub1, ub2, ub3, lhs, dm, dp, cxh,
                cx, cy, pad, s, u0, u1, bx, by, bys, natural, pk, cyh, sh, upk, uh, edge, rolled0, rolled1, turn, gsend, ga, gb, last_send, last_a, last_b,
                in_sem, bar_send, bar_recv):
    nrow, ncol = grid
    rb, cb = dm.shape
    nb = rb // LANES
    row, col = lax.axis_index("row"), lax.axis_index("col")
    down, above = lax.rem(row + 1, nrow), lax.rem(row + nrow - 1, nrow)
    right, left = lax.rem(col + 1, ncol), lax.rem(col + ncol - 1, ncol)
    fields = [u0, u1, u0]
    basis = [ub0, ub1, ub2, ub3]
    used = [0]
    sent = []

    def send(src, dst, row_to, col_to):
        slot = used[0]
        used[0] += 1
        copy = pltpu.make_async_remote_copy(
            src_ref=src, dst_ref=dst, send_sem=bar_send.at[slot], recv_sem=bar_recv.at[slot],
            device_id=(row_to, col_to), device_id_type=MESH)
        copy.start()
        sent.append(copy)
        return copy

    def done(copy):
        copy.wait_send()
        sent[:] = [c for c in sent if c is not copy]

    barrier = pltpu.get_barrier_semaphore()
    for d in range(1, nrow):
        pl.semaphore_signal(barrier, inc=1, device_id=(lax.rem(row + d, nrow), col), device_id_type=MESH)
    for d in range(1, ncol):
        pl.semaphore_signal(barrier, inc=1, device_id=(row, lax.rem(col + d, ncol)), device_id_type=MESH)

    local = []
    for n, (src, dst) in enumerate(((cy_in, cy), (cx_in, cx.at[pl.ds(8, rb)]), (pad_in, pad))):
        copy = pltpu.make_async_copy(src, dst, in_sem.at[n])
        copy.start()
        local.append(copy)
    fill = []
    for k in range(RHS):
        copy = pltpu.make_async_copy(rhs.at[k], u0.at[pl.ds(1, rb), k, :], in_sem.at[3 + k])
        copy.start()
        fill.append(copy)

    local[0].wait()
    pk[0] = jnp.transpose(cy[:, cb - LANES :])[LANES - 8 :]
    local[1].wait()
    pl.semaphore_wait(barrier, nrow + ncol - 2)
    got_cx = send(cx.at[pl.ds(rb, 8)], cxh, down, col)
    got_cy = send(pk.at[0], cyh, row, right)
    local[2].wait()
    cx[0:8] = jnp.zeros_like(cxh)
    chunk = 32

    def scale_nodes(r, height, width, left_known):
        here = pl.ds(r, height)
        cond_y = cy[here, :width]
        moved = pltpu.roll(cond_y, 1, axis=1)
        if left_known:
            first = jnp.where(lane_of((height, LANES)) == 0, natural[0, here], moved[:, :LANES])
            moved = jnp.concatenate([first, moved[:, LANES:]], axis=1) if width > LANES else first
        pads = pad[here, :width].astype(F32)
        free = 1.0 - pads
        diagonal = free * (cx[pl.ds(r + 8, height), :width] + cx[pl.ds(r + 7, height), :width] + cond_y + moved) + pads
        root = lax.rsqrt(diagonal)
        dm[here, :width] = root
        dp[here, :width] = diagonal * root
        s[pl.ds(r + 8, height), :width] = free * root

    for r in range(0, rb, chunk):
        scale_nodes(r, chunk, cb, False)

    lane = lane_of((RHS, LANES))

    def store_split(j, r, value, start=0):
        high, low = split(value)
        lanes = slice(start, start + value.shape[1])
        basis[j][r, :RHS, lanes] = high
        basis[j][r, RHS:, lanes] = low

    for copy in fill:
        copy.wait()
    rolled0[0, 0] = u0[1]

    def inner(i, carry):
        for t in range(BEGIN):
            at = i * BEGIN + t
            value = u0[at + 1, :, LANES:] * dm[pl.ds(at, 1), :][:, LANES:]
            u0[at + 1, :, LANES:] = value
            store_split(0, at, value, LANES)
        return carry

    lax.fori_loop(0, rb // BEGIN, inner, 0)

    got_cx.wait_recv()
    got_cy.wait_recv()
    cx[0:8] = cxh[...] * stay_scalar(row > 0)
    cyh[...] = cyh[...] * stay_scalar(col > 0)
    natural[0] = jnp.transpose(jnp.broadcast_to(cyh[7:8, :], (LANES, rb)))
    scale_nodes(0, 8, cb, True)
    for r in range(0, rb, chunk):
        scale_nodes(r, chunk, LANES, True)
    pk[1] = jnp.transpose(s[pl.ds(8, rb), 0:LANES])[:8]
    pk[2] = jnp.transpose(s[pl.ds(8, rb), cb - LANES : cb])[LANES - 8 :]
    got_s = [
        send(s.at[pl.ds(rb, 8)], s.at[pl.ds(0, 8)], down, col),
        send(s.at[pl.ds(8, 8)], s.at[pl.ds(rb + 8, 8)], above, col),
        send(pk.at[1], sh.at[1], row, left),
        send(pk.at[2], sh.at[0], row, right),
    ]

    def send_columns(j, b):
        coming[j, b] = [
            send(upk.at[j, 0, b], uh.at[j, 1, b], row, left),
            send(upk.at[j, 1, b], uh.at[j, 0, b], row, right),
        ]

    def send_row(j, last):
        field = fields[j]
        if last:
            coming[j, "above"] = [send(field.at[rb], edge.at[j, 0], down, col)]
        else:
            coming[j, "below"] = [send(field.at[1], edge.at[j, 1], above, col)]

    def arrive(j, key):
        for copy in coming[j, key]:
            copy.wait_recv()

    coming = {}
    even_lane = (lane & 1) == 0

    def pack_edges(first, last, r, parity, held):
        ends = pltpu.roll(jnp.where(lane == LANES - 1, last, first), r, axis=1)
        here = (lane == r) | (lane == ((r - 1) & (LANES - 1)))
        return tuple(jnp.where(here, ends, held[n]) if n == parity else held[n] for n in range(2))

    def keep_edges(j, b, held):
        upk[j, 0, b] = jnp.where(even_lane, held[0], held[1])
        upk[j, 1, b] = jnp.where(even_lane, held[1], held[0])

    empty = (jnp.zeros((RHS, LANES), F32), jnp.zeros((RHS, LANES), F32))

    top = rolled0[0, 0] * dm[0:1, :]
    u0[1, :, LANES:] = top[:, LANES:]
    store_split(0, 0, top[:, LANES:], LANES)
    for b in range(nb):
        def begin(i, held, b=b):
            for t in range(BEGIN):
                r = i * BEGIN + t
                at = b * LANES + r
                value = u0[at + 1, :, :LANES] * dm[pl.ds(at, 1), :][:, :LANES]
                u0[at + 1, :, :LANES] = value
                store_split(0, at, value)
                held = pack_edges(value, u0[at + 1, :, cb - LANES :], r, t % 2, held)
            return held

        keep_edges(0, b, lax.fori_loop(0, LANES // BEGIN, begin, empty))
        send_columns(0, b)
        if b == 0:
            send_row(0, False)
    send_row(0, True)

    lows = STEPS + 1

    def gram_rows(left_blocks, right_blocks, rows):
        def operand(blocks):
            parts = [
                jnp.concatenate(
                    [basis[n % lows][r, n // lows * RHS : (n // lows + 1) * RHS, :] for n in blocks], axis=0)
                for r in rows
            ]
            return jnp.concatenate(parts, axis=1)

        return gram_dot(operand(left_blocks), operand(right_blocks))

    def gram_loop(left_blocks, right_blocks):
        def body(i, total):
            return total + gram_rows(left_blocks, right_blocks, [i * GROUP + t for t in range(GROUP)])

        shape = (len(left_blocks) * RHS, len(right_blocks) * RHS)
        return lax.fori_loop(0, rb // GROUP, body, jnp.zeros(shape, F32))

    def keep_moment(k, value):
        if k < 2 * STEPS - 1:
            gsend[0, :, k * RHS : (k + 1) * RHS] = value
        else:
            gsend[2, :, :RHS] = value

    gsend[...] = jnp.zeros_like(gsend)
    place = lax.broadcasted_iota(jnp.int32, turn.shape, 0) & (LANES - 1)
    spot = lane_of(turn.shape)
    comes = jnp.where(spot < LANES, spot + 1, spot - 1) & (LANES - 1)
    turn[...] = jnp.where(place == comes, 1.0, 0.0).astype(BF16)
    total = gram_loop([0], [0, lows])
    keep_moment(0, total[:, :RHS] + 2.0 * total[:, RHS:])

    for copy in got_s:
        copy.wait_recv()
    s[pl.ds(rb + 8, 8)] = s[pl.ds(rb + 8, 8)] * stay_scalar(row < nrow - 1)
    sh[1] = sh[1] * stay_scalar(col < ncol - 1)
    natural[1] = jnp.transpose(jnp.broadcast_to(sh[0, 7:8, :], (LANES, rb)))
    natural[2] = jnp.transpose(jnp.broadcast_to(sh[1, 0:1, :], (LANES, rb)))
    for r in range(0, rb, chunk):
        here = pl.ds(r, chunk)
        mine = s[pl.ds(r + 8, chunk)]
        moved = pltpu.roll(mine, cb - 1, axis=1)
        last = jnp.where(lane_of((chunk, LANES)) == LANES - 1, natural[2, here], moved[:, cb - LANES :])
        side = cy[here] * mine * jnp.concatenate([moved[:, : cb - LANES], last], axis=1)
        by[here] = side
        moved = pltpu.roll(side, 1, axis=1)
        first = natural[0, here] * natural[1, here] * mine[:, :LANES]
        first = jnp.where(lane_of((chunk, LANES)) == 0, first, moved[:, :LANES])
        bys[here] = jnp.concatenate([first, moved[:, LANES:]], axis=1)
        bx[here] = cx[pl.ds(r + 7, chunk)] * s[pl.ds(r + 7, chunk)] * mine
    bx[rb : rb + 1] = cx[rb + 7 : rb + 8] * s[rb + 7 : rb + 8] * s[rb + 8 : rb + 9]

    def shift_rows(j, start, rolled):
        parts = []
        for t in range(UNROLL):
            for c in range(0, cb, LANES):
                parts.append(jnp.concatenate(
                    [basis[j][start + t, :RHS, c : c + LANES], basis[j][start + t, RHS:, c : c + LANES]], axis=1))
        out = jnp.dot(jnp.concatenate(parts, axis=0), turn[...], preferred_element_type=F32)
        n = 0
        for t in range(UNROLL):
            for c in range(0, cb, LANES):
                for m in range(2):
                    rolled[t, m, :, c : c + LANES] = out[n : n + RHS, m * LANES : (m + 1) * LANES]
                n += RHS

    shift_rows(0, 0, rolled0)

    def start_reduce(part, slots, me, size, along_row):
        got = []
        for d in range(1, size):
            to = lax.rem(me + d, size)
            got.append(send(part, slots.at[me], *((to, col) if along_row else (row, to))))
        slots[me] = part[...]
        return got

    def finish_reduce(got, slots, size):
        for copy in got:
            copy.wait_recv()
        parts = [slots[n] for n in range(size)]
        while len(parts) > 1:
            parts = [parts[n] + parts[n + 1] for n in range(0, len(parts), 2)]
        return parts[0]

    for j in range(STEPS):
        if j == STEPS - 1:
            early = start_reduce(gsend.at[0], ga, row, nrow, True)
        source = fields[j]
        final = j == STEPS - 1
        if final:
            arrive(j, "above")
            source[0] = edge[j, 0]
        else:
            source[0] = jnp.zeros((RHS, cb), F32)
        pair = jnp.zeros((2 * RHS, 2 * RHS), F32)
        for b in range(nb):
            if final and b == 1:
                gsend[1] = finish_reduce(early, ga, nrow)
                early = start_reduce(gsend.at[1], gb, col, ncol, False)
            arrive(j, b)
            if b == nb - 1:
                arrive(j, "below")
                source[rb + 1] = edge[j, 1]
            before = pltpu.roll(uh[j, 0, b], 1, axis=1)
            after = pltpu.roll(uh[j, 1, b], LANES - 1, axis=1)
            outside = (jnp.where(even_lane, before, after), jnp.where(even_lane, after, before))

            def apply(i, held, b=b, outside=outside, source=source, j=j, final=final):
                held = list(held)
                base = b * LANES + i * 2 * UNROLL
                if final:
                    ready = jnp.maximum(base - 2 * UNROLL, 0)
                    fresh = gram_rows([j, lows + j], [j + 1, lows + j + 1], [ready + t for t in range(2 * UNROLL)])
                    held[0] = held[0] + jnp.where(base > 0, fresh, 0.0)
                else:
                    for t in range(2 * UNROLL):
                        r = (i - 1) * 2 * UNROLL + t
                        at = jnp.maximum(b * LANES + r, 0) + 1
                        first, last = fields[j + 1][at, :, :LANES], fields[j + 1][at, :, cb - LANES :]
                        held = pack_edges(first, last, r, t % 2, held)
                for half, (now, later) in enumerate(((rolled0, rolled1), (rolled1, rolled0))):
                    shift_rows(j, jnp.minimum(base + (half + 1) * UNROLL, rb - UNROLL), later)
                    for t in range(UNROLL):
                        r = (i * 2 + half) * UNROLL + t
                        at = b * LANES + r
                        total = bx[pl.ds(at, 1), :] * source[at] + bx[pl.ds(at + 1, 1), :] * source[at + 2]
                        ends = pltpu.roll(outside[t % 2], (LANES - r) & (LANES - 1), axis=1)
                        ahead = tiles_of(now[t, 0]) + [ends]
                        ahead = [jnp.where(lane == LANES - 1, ahead[c + 1], ahead[c]) for c in range(len(ahead) - 1)]
                        behind = [ends] + tiles_of(now[t, 1])
                        behind = [jnp.where(lane == 0, behind[c], behind[c + 1]) for c in range(len(behind) - 1)]
                        total = total + by[pl.ds(at, 1), :] * jnp.concatenate(ahead, axis=1)
                        value = total + bys[pl.ds(at, 1), :] * jnp.concatenate(behind, axis=1)
                        store_split(j + 1, at, value)
                        if not final:
                            fields[j + 1][at + 1] = value
                return tuple(held)

            trips = LANES // (2 * UNROLL)
            if final:
                pair, = lax.fori_loop(0, trips, apply, (pair,))
            else:
                held = lax.fori_loop(0, trips, apply, empty)
                for t in range(2 * UNROLL):
                    r = LANES - 2 * UNROLL + t
                    at = b * LANES + r + 1
                    first, last = fields[j + 1][at, :, :LANES], fields[j + 1][at, :, cb - LANES :]
                    held = pack_edges(first, last, r, t % 2, held)
                if b == 0:
                    arrive(j, "above")
                    value = fields[j + 1][1] + bx[0:1, :] * edge[j, 0]
                    fields[j + 1][1] = value
                    store_split(j + 1, 0, value)
                    held = pack_edges(value[:, :LANES], value[:, cb - LANES :], 0, 0, held)
                keep_edges(j + 1, b, held)
                send_columns(j + 1, b)
                if b == 0:
                    send_row(j + 1, False)
        if not final:
            send_row(j + 1, True)
            for key in ("above", "below"):
                done(coming[j, key][0])
            total = gram_loop([j, lows + j, j + 1], [j + 1, lows + j + 1])
            shift_rows(j + 1, 0, rolled0)
            even = total[2 * RHS :]
            keep_moment(2 * j + 2, even[:, :RHS] + 2.0 * even[:, RHS:])
        else:
            rows = [rb - 2 * UNROLL + t for t in range(2 * UNROLL)]
            total = pair + gram_rows([j, lows + j], [j + 1, lows + j + 1], rows)
        keep_moment(2 * j + 1, total[:RHS, :RHS] + total[:RHS, RHS:] + total[RHS : 2 * RHS, :RHS])
    half = RHS // 2
    spread = pltpu.roll(gsend[2], 0, axis=1, stride=RHS, stride_axis=0)
    last_send[0] = jnp.concatenate(
        [jnp.sum(spread[n : n + half], axis=0, keepdims=True) for n in (0, half)], axis=0)
    late = start_reduce(last_send.at[0], last_a, row, nrow, True)

    wide = lane_of((RHS, LANES))

    def turned(total):
        flip = jnp.transpose(total)
        flip = jnp.concatenate([flip[k * RHS : (k + 1) * RHS] for k in range(LANES // RHS)], axis=1)
        return 0.5 * (total + flip)

    moments = turned(finish_reduce(early, gb, ncol))
    stiff = moments - pltpu.roll(moments, LANES - RHS, axis=1)
    order = STEPS * RHS
    blocks = [stiff] + [pltpu.roll(stiff, LANES - RHS * n, axis=1) for n in range(1, STEPS)] + [moments]
    stack = jnp.concatenate([jnp.where(wide < order, v, 0.0) for v in blocks], axis=0)
    stack = eliminate(stack, order - RHS, 0)
    last_send[1] = finish_reduce(late, last_a, nrow)
    late = start_reduce(last_send.at[1], last_b, col, ncol, False)
    last = finish_reduce(late, last_b, ncol)
    backward = [
        pltpu.roll(jnp.broadcast_to(last[n : n + 1], (half, LANES)), RHS, axis=1, stride=RHS, stride_axis=0)
        for n in range(2)
    ]
    last = jnp.concatenate([v[half - 1 - n : half - n] for v in backward for n in range(half)], axis=0)
    last = turned(last)
    inside = (wide >= order - RHS) & (wide < order)
    last = jnp.where(inside, pltpu.roll(last, order - RHS, axis=1), 0.0)
    stack = jnp.concatenate([stack[:RHS] - last, stack[RHS:]], axis=0)
    solved = eliminate(stack, RHS, order - RHS)
    unit = jnp.where(wide == lax.broadcasted_iota(jnp.int32, (RHS, LANES), 0), 1.0, 0.0)
    remain = unit - solved + pltpu.roll(solved, RHS, axis=1)
    coef = jnp.concatenate([solved, remain], axis=0)
    high = coef.astype(BF16).astype(F32)
    low = coef - high
    lhs[...] = jnp.concatenate([high + pltpu.roll(high, LANES // 2, axis=1), low], axis=0).astype(BF16)

    for copy in sent:
        copy.wait_send()


def combine_kernel(ub0, ub1, ub2, ub3, lhs, dm, dp, x_out, r_out, x_buf, r_buf, sem):
    rb, cb = dm.shape
    block = 64
    coef = lhs[...]
    started = []
    for n in range(rb // block):
        def body(i, carry, n=n):
            rows = [n * block + i * ROWS + t for t in range(ROWS)]
            out = jnp.dot(coef, jnp.concatenate(
                [
                    jnp.concatenate([v[r, m : m + RHS, :] for m in (0, RHS) for v in (ub0, ub1, ub2, ub3)], axis=0)
                    for r in rows
                ], axis=1), preferred_element_type=F32)
            for t, r in enumerate(rows):
                part = out[:, t * cb : (t + 1) * cb]
                x_buf[r] = (part[:RHS] + part[2 * RHS : 3 * RHS]) * dm[pl.ds(r, 1), :]
                r_buf[r] = (part[RHS : 2 * RHS] + part[3 * RHS :]) * dp[pl.ds(r, 1), :]
            return carry

        lax.fori_loop(0, block // ROWS, body, 0)
        here = pl.ds(n * block, block)
        for k in range(RHS):
            for m, (buf, out) in enumerate(((x_buf, x_out), (r_buf, r_out))):
                copy = pltpu.make_async_copy(buf.at[here, k, :], out.at[k, here, :], sem.at[n, m, k])
                copy.start()
                started.append(copy)
    for copy in started:
        copy.wait()


def shards(nrow, ncol, right_side, cond_x, cond_y, pad_mask):
    rb, cb = cond_x.shape
    nb = rb // LANES
    sends = 2 + 4 + (2 * nb + 2) * STEPS + 2 * (nrow - 1) + 2 * (ncol - 1)
    hbm = pl.BlockSpec(memory_space=pltpu.HBM)
    vmem = pl.BlockSpec(memory_space=pltpu.VMEM)
    field = pltpu.VMEM((rb + 2, RHS, cb), F32)
    *kept, = pl.pallas_call(
        functools.partial(main_kernel, (nrow, ncol)),
        out_shape=(
            *[pltpu.VMEM((rb, 2 * RHS, cb), BF16)] * (STEPS + 1), pltpu.VMEM((4 * RHS, LANES), BF16),
            pltpu.VMEM((rb, cb), F32), pltpu.VMEM((rb, cb), F32),
        ),
        in_specs=[hbm] * 4,
        out_specs=(vmem,) * (STEPS + 4),
        scratch_shapes=[
            pltpu.VMEM((8, cb), F32),
            pltpu.VMEM((rb + 8, cb), F32), pltpu.VMEM((rb, cb), F32), pltpu.VMEM((rb, cb), jnp.int32),
            pltpu.VMEM((rb + 16, cb), F32), field, field,
            pltpu.VMEM((rb + 8, cb), F32), pltpu.VMEM((rb, cb), F32), pltpu.VMEM((rb, cb), F32),
            pltpu.VMEM((3, rb, LANES), F32), pltpu.VMEM((3, 8, rb), F32),
            pltpu.VMEM((8, rb), F32), pltpu.VMEM((2, 8, rb), F32),
            pltpu.VMEM((STEPS, 2, nb, RHS, LANES), F32), pltpu.VMEM((STEPS, 2, nb, RHS, LANES), F32),
            pltpu.VMEM((STEPS, 2, RHS, cb), F32), pltpu.VMEM((UNROLL, 2, RHS, cb), F32), pltpu.VMEM((UNROLL, 2, RHS, cb), F32),
            pltpu.VMEM((2 * LANES, 2 * LANES), BF16),
            pltpu.VMEM((3, RHS, LANES), F32), pltpu.VMEM((nrow, RHS, LANES), F32), pltpu.VMEM((ncol, RHS, LANES), F32),
            pltpu.VMEM((2, 2, LANES), F32), pltpu.VMEM((nrow, 2, LANES), F32), pltpu.VMEM((ncol, 2, LANES), F32),
            pltpu.SemaphoreType.DMA((3 + RHS,)), pltpu.SemaphoreType.DMA((sends,)), pltpu.SemaphoreType.DMA((sends,)),
        ],
        compiler_params=pltpu.CompilerParams(
            collective_id=0, has_side_effects=True, vmem_limit_bytes=24 * 2**20),
    )(*(pltpu.with_memory_space_constraint(v, pltpu.HBM) for v in (right_side, cond_x, cond_y, pad_mask)))
    out = jax.ShapeDtypeStruct((RHS, rb, cb), F32)
    return pl.pallas_call(
        combine_kernel,
        out_shape=(out, out),
        in_specs=[vmem] * (STEPS + 4),
        out_specs=(hbm, hbm),
        scratch_shapes=[
            pltpu.VMEM((rb, RHS, cb), F32), pltpu.VMEM((rb, RHS, cb), F32),
            pltpu.SemaphoreType.DMA((rb // 64, 2, RHS)),
        ],
        compiler_params=pltpu.CompilerParams(vmem_limit_bytes=14 * 2**20),
    )(*kept)


def solution(mesh):
    nrow, ncol = mesh.shape["row"], mesh.shape["col"]
    field, plane = P(None, "row", "col"), P("row", "col")
    return jax.shard_map(
        functools.partial(shards, nrow, ncol), mesh=mesh,
        in_specs=(field, plane, plane, plane), out_specs=(field, field), check_vma=False,
    )
```
